64 devices in a mesh: dp: 4 (over x, y), ep: 16 (over z, core).
Axes of the slice: x: 2, y: 2, z: 8, core: 2. Of those that a mesh axis runs over, the one named last changes fastest.
The devices are a block of a 4x4x8 slice.
Arguments:
- x_in: bfloat16 [65536, 1024], P(('dp', 'ep')), parts along dimension 0
- norm_gain: bfloat16 [1024], replicated
- w_router: bfloat16 [1024, 32], replicated
- expert_ids: int32 [65536, 8], P(('dp', 'ep')), parts along dimension 0
- w_gate: bfloat16 [32, 1024, 512], P('ep')
- w_up: bfloat16 [32, 1024, 512], P('ep')
- w_down: bfloat16 [32, 512, 1024], P('ep')
Outputs:
- output: bfloat16 [65536, 1024], P(('dp', 'ep')), parts along dimension 0
There are 4 independent parts. The reference program is written for one: setup_inputs(seed, part) draws one part's arguments, and reference() takes and returns one part's arrays. A program takes and returns all parts, laid end to end along the dimension named above; an argument that names none is the same for every part.
All inputs are finite; a program needn't handle non-finite values.
Results may differ from the reference program's by a relative error of at most 0.001.
Values are sent between devices in bfloat16 or wider.
A program may use at most 768 MiB of HBM per device.

```python
import jax
import jax.numpy as jnp
from jax import lax

HIDDEN = 1024
EXPERT_FF = 512
EXPERTS = 32
TOP_K = 8
TOKENS = 1024
GROUP_SIZE = 16

EPS = 1e-6
CAP_DEV = 2 * TOKENS * TOP_K // EXPERTS
HOT_COUNT = EXPERTS // 4
COLD_LEFT = TOKENS * TOP_K - HOT_COUNT * CAP_DEV
COLD_BASE = COLD_LEFT // (EXPERTS - HOT_COUNT)
COLD_EXTRA = COLD_LEFT % (EXPERTS - HOT_COUNT)
ROW_LIMIT = GROUP_SIZE * CAP_DEV


def draw_device(hot_flag, key):
    key_rank, key_rows, key_cols = jax.random.split(key, 3)
    expert_range = jnp.arange(EXPERTS, dtype=jnp.int32)
    noise = jax.random.randint(key_rank, (EXPERTS,), 0, EXPERTS, dtype=jnp.int32)
    score = (1 - hot_flag) * (EXPERTS * EXPERTS) + noise * EXPERTS + expert_range
    rank = jnp.argsort(jnp.argsort(score))
    counts = jnp.where(rank < HOT_COUNT, CAP_DEV, COLD_BASE + (rank - HOT_COUNT < COLD_EXTRA).astype(jnp.int32))
    bounds = jnp.cumsum(counts).astype(jnp.int32)
    flat_ids = jnp.searchsorted(bounds, jnp.arange(TOKENS * TOP_K, dtype=jnp.int32), side="right").astype(jnp.int32)
    table = flat_ids.reshape(TOP_K, TOKENS).T
    table = jax.random.permutation(key_rows, table, axis=0)
    col_score = jax.random.randint(key_cols, (TOKENS, TOP_K), 0, TOP_K, dtype=jnp.int32) * TOP_K + jnp.arange(TOP_K, dtype=jnp.int32)
    col_order = jnp.argsort(col_score, axis=1)
    return jnp.take_along_axis(table, col_order, axis=1)


def draw_routes(key):
    key_hot, key_dev = jax.random.split(key)
    hot_order = jax.random.permutation(key_hot, EXPERTS)
    hot_flag = (jnp.argsort(hot_order) < HOT_COUNT).astype(jnp.int32)
    dev_keys = jax.random.split(key_dev, GROUP_SIZE)
    routes = jax.vmap(draw_device, in_axes=(None, 0))(hot_flag, dev_keys)
    return routes.reshape(GROUP_SIZE * TOKENS, TOP_K).astype(jnp.int32)


def setup_inputs(seed: int = 0, part: int = 0) -> dict:
    shared = jax.random.split(jax.random.key(seed), 5)
    own = jax.random.split(jax.random.fold_in(jax.random.key(seed + 1), part), 2)
    x_in = (0.5 * jax.random.normal(own[0], (GROUP_SIZE * TOKENS, HIDDEN), jnp.float32)).astype(jnp.bfloat16)
    norm_gain = jax.random.uniform(shared[0], (HIDDEN,), jnp.float32, 0.5, 1.5).astype(jnp.bfloat16)
    w_router = (2.0 * HIDDEN ** -0.5 * jax.random.normal(shared[1], (HIDDEN, EXPERTS), jnp.float32)).astype(jnp.bfloat16)
    w_gate = (HIDDEN ** -0.5 * jax.random.normal(shared[2], (EXPERTS, HIDDEN, EXPERT_FF), jnp.float32)).astype(jnp.bfloat16)
    w_up = (HIDDEN ** -0.5 * jax.random.normal(shared[3], (EXPERTS, HIDDEN, EXPERT_FF), jnp.float32)).astype(jnp.bfloat16)
    w_down = (1.5 * EXPERT_FF ** -0.5 * jax.random.normal(shared[4], (EXPERTS, EXPERT_FF, HIDDEN), jnp.float32)).astype(jnp.bfloat16)
    expert_ids = draw_routes(own[1])
    return {"x_in": x_in, "norm_gain": norm_gain, "w_router": w_router, "expert_ids": expert_ids, "w_gate": w_gate, "w_up": w_up, "w_down": w_down}


def reference(x_in, norm_gain, w_router, expert_ids, w_gate, w_up, w_down):
    resid = x_in.astype(jnp.float32)
    mean_sq = jnp.mean(resid * resid, axis=-1, keepdims=True)
    normed = (resid * lax.rsqrt(mean_sq + EPS) * norm_gain.astype(jnp.float32)).astype(jnp.bfloat16)
    logits = jnp.dot(normed, w_router, preferred_element_type=jnp.float32)
    router_p = jax.nn.softmax(logits, axis=-1)
    picked = jnp.take_along_axis(router_p, expert_ids, axis=1)
    gates = picked / jnp.sum(picked, axis=1, keepdims=True)
    total = x_in.shape[0]

    def one_expert(moe_sum, inputs):
        expert, gate_w, up_w, down_w = inputs
        hits = expert_ids == expert
        weight = jnp.sum(jnp.where(hits, gates, 0.0), axis=1)
        rows = jnp.nonzero(jnp.any(hits, axis=1), size=ROW_LIMIT, fill_value=total)[0]
        sel_rows = jnp.take(normed, rows, axis=0, mode="fill", fill_value=0)
        gate_val = jnp.dot(sel_rows, gate_w, preferred_element_type=jnp.float32)
        up_val = jnp.dot(sel_rows, up_w, preferred_element_type=jnp.float32)
        hidden_act = (jax.nn.silu(gate_val) * up_val).astype(jnp.bfloat16)
        out_rows = jnp.dot(hidden_act, down_w, preferred_element_type=jnp.float32).astype(jnp.bfloat16)
        row_w = jnp.take(weight, rows, mode="fill", fill_value=0)
        moe_sum = moe_sum.at[rows].add(out_rows.astype(jnp.float32) * row_w[:, None], mode="drop")
        return moe_sum, None

    start_sum = jnp.zeros((total, HIDDEN), jnp.float32)
    moe_sum = lax.scan(one_expert, start_sum, (jnp.arange(EXPERTS, dtype=jnp.int32), w_gate, w_up, w_down))[0]
    return (resid + moe_sum).astype(jnp.bfloat16)
```

```python
import functools
import math

import jax
import jax.numpy as jnp
from jax import lax
from jax.experimental import pallas as pl
from jax.experimental.pallas import tpu as pltpu
from jax.sharding import PartitionSpec as P

EPS = 1e-6
MESH = pl.DeviceIdType.MESH
LANES = 128
CORES = 2
LAG = 3


def kernel(nz, yspan, x_ref, gain_ref, router_ref, ids_ref, gate_in, up_in, down_in, out_ref, gate_land, up_land, down_land,
           normed, total, weight, hidden, gate_buf, up_buf, down_buf, send_z, send_xy, send_sib, recv, load_sem):
    dp, ep = lax.axis_index("dp"), lax.axis_index("ep")
    z, c = ep // CORES, ep % CORES
    a, b = (dp // yspan) % 2, dp % 2
    relay = (a + b + c) % 2
    right = (dp, ((z + 1) % nz) * CORES + c)
    left = (dp, ((z + nz - 1) % nz) * CORES + c)
    x_peer = (dp + yspan * (1 - 2 * a), ep)
    y_peer = (dp + 1 - 2 * b, ep)
    sibling = (dp, z * CORES + 1 - c)
    tokens, width = x_ref.shape
    experts = router_ref.shape[1]
    batches = nz - 1
    items = 4 * nz
    arrays = ((gate_in, gate_land, gate_buf), (up_in, up_land, up_buf), (down_in, down_land, down_buf))

    def send(src, dst, send_sem, recv_sem, device):
        return pltpu.make_async_remote_copy(src_ref=src, dst_ref=dst, send_sem=send_sem, recv_sem=recv_sem, device_id=device, device_id_type=MESH)

    barrier = pltpu.get_barrier_semaphore()
    for peer in (right, left, x_peer, y_peer, sibling):
        pl.semaphore_signal(barrier, inc=1, device_id=peer, device_id_type=MESH)
    pl.semaphore_wait(barrier, 5)

    for j in range(2):
        for k, (own, land, _) in enumerate(arrays):
            @pl.when(relay == 0)
            def _():
                send(own.at[j], land.at[c, z, j], send_z.at[0, k, j], recv.at[k, c, z, j], right).start()
                send(own.at[1 - j], land.at[c, z, 1 - j], send_z.at[1, k, j], recv.at[k, c, z, 1 - j], left).start()
            send(own.at[j], land.at[c, z, j], send_sib.at[k, 0, j], recv.at[k, c, z, j], sibling).start()

    tile = min(128, tokens)

    @pl.loop(0, tokens // tile)
    def _(step):
        rows = pl.ds(pl.multiple_of(step * tile, tile), tile)
        resid = x_ref[rows, :].astype(jnp.float32)
        mean_sq = jnp.mean(resid * resid, axis=-1, keepdims=True)
        row = (resid * lax.rsqrt(mean_sq + EPS) * gain_ref[...].astype(jnp.float32)).astype(jnp.bfloat16)
        normed[rows, :] = row
        total[rows, :] = resid
        logits = jnp.dot(row, router_ref[...], preferred_element_type=jnp.float32)
        ids = ids_ref[rows, :]
        lane = lax.broadcasted_iota(jnp.int32, (tile, experts), 1)
        chosen = lane == ids[:, 0:1]
        for j in range(1, ids.shape[1]):
            chosen = chosen | (lane == ids[:, j:j + 1])
        shifted = jnp.exp(logits - jnp.max(logits, axis=-1, keepdims=True))
        prob = shifted / jnp.sum(shifted, axis=-1, keepdims=True)
        picked = jnp.where(chosen, prob, 0.0)
        gates = picked / jnp.sum(picked, axis=-1, keepdims=True)
        for e in range(experts):
            weight[e, rows, :] = jnp.broadcast_to(gates[:, e:e + 1], (tile, LANES))

    def place(n, side):
        dist, first = 1 + n // 2, n % 2
        return (z + nz + (2 * side - 1) * dist) % nz, first + side - 2 * first * side

    def exchange(n, k):
        _, land, _ = arrays[k]
        first = n % 2
        for side in range(2):
            zs, j = place(n, side)
            chunk, sem = land.at[c, zs, j], recv.at[k, c, zs, j]
            send(chunk, chunk, send_sib.at[k, n + 1, side], sem, sibling).wait_recv()

            @pl.when((relay == 0) & (n < batches - 2))
            def _():
                send(chunk, chunk, send_z.at[side, k, n + 2], sem, (right, left)[side]).start()

            @pl.when((relay == 0) & (first == side))
            def _():
                send(chunk, chunk, send_xy.at[0, k, n], sem, x_peer).start()

            @pl.when((relay == 0) & (first != side))
            def _():
                send(chunk, chunk, send_xy.at[1, k, n], sem, y_peer).start()
            send(chunk, chunk, send_sib.at[k, n + 1, side], sem, sibling).start()

    @pl.loop(0, items)
    def _(i):
        at = i - LAG * relay
        live = (at >= 0) & (at < 4 * batches)
        for k, phase in enumerate((0, 2, 3)):
            @pl.when(live & ((at + 4) % 4 == phase))
            def _():
                exchange((at + 4) // 4 - 1, k)

        m, q = i // 4, i % 4
        side, other = q % 2, (q // 2 + relay) % 2
        cls = (c + other) % 2
        dist, first = (m + 1) // 2, (m + 1) % 2
        zs = (z + nz + (2 * side - 1) * dist) % nz
        j = first + side - 2 * first * side
        slot = i % 2

        @pl.when(other == 1)
        def _():
            for k, (_, land, _) in enumerate(arrays):
                chunk = land.at[cls, zs, j]
                send(chunk, chunk, send_sib.at[k, 0, 0], recv.at[k, cls, zs, j], sibling).wait_recv()

        native = (m == 0) & (other == 0)

        @pl.when(native)
        def _():
            for k, (own, _, buf) in enumerate(arrays):
                pltpu.make_async_copy(own.at[j], buf.at[slot], load_sem.at[k]).start()

        @pl.when(jnp.logical_not(native))
        def _():
            for k, (_, land, buf) in enumerate(arrays):
                pltpu.make_async_copy(land.at[cls, zs, j], buf.at[slot], load_sem.at[k]).start()

        for k in range(2):
            own, _, buf = arrays[k]
            pltpu.make_async_copy(own.at[0], buf.at[slot], load_sem.at[k]).wait()

        span = min(512, tokens)

        @pl.loop(0, tokens // span)
        def _(step):
            rows = pl.ds(pl.multiple_of(step * span, span), span)
            row = normed[rows, :]
            gate_val = jnp.dot(row, gate_buf[slot], preferred_element_type=jnp.float32)
            up_val = jnp.dot(row, up_buf[slot], preferred_element_type=jnp.float32)
            hidden[rows, :] = (jax.nn.silu(gate_val) * up_val).astype(jnp.bfloat16)

        pltpu.make_async_copy(down_in.at[0], down_buf.at[slot], load_sem.at[2]).wait()
        expert = (zs * CORES + cls) * 2 + j

        @pl.loop(0, tokens // span)
        def _(step):
            rows = pl.ds(pl.multiple_of(step * span, span), span)
            y = jnp.dot(hidden[rows, :], down_buf[slot], preferred_element_type=jnp.float32).astype(jnp.bfloat16).astype(jnp.float32)
            scale = jnp.concatenate([weight[expert, rows, :]] * (width // LANES), axis=1)
            total[rows, :] += jnp.where(scale != 0.0, scale * y, 0.0)

    @pl.loop(0, tokens // tile)
    def _(step):
        rows = pl.ds(pl.multiple_of(step * tile, tile), tile)
        out_ref[rows, :] = total[rows, :].astype(jnp.bfloat16)

    for k, (own, land, _) in enumerate(arrays):
        @pl.when(relay == 0)
        def _():
            @pl.loop(0, batches)
            def _(n):
                for side in range(2):
                    send(own.at[0], land.at[0, 0, 0], send_z.at[side, k, n], recv.at[k, 0, 0, 0], right).wait_send()
                    send(own.at[0], land.at[0, 0, 0], send_xy.at[side, k, n], recv.at[k, 0, 0, 0], right).wait_send()

        @pl.loop(0, batches + 1)
        def _(n):
            for side in range(2):
                send(own.at[0], land.at[0, 0, 0], send_sib.at[k, n, side], recv.at[k, 0, 0, 0], sibling).wait_send()


def solution(mesh):
    yspan = math.isqrt(mesh.shape["dp"])
    nz = mesh.shape["ep"] // CORES

    def local_block(x_in, norm_gain, w_router, expert_ids, w_gate, w_up, w_down):
        tokens, width = x_in.shape
        experts = w_router.shape[1]
        ff = w_gate.shape[2]
        batches = nz - 1
        vmem, anywhere = pl.BlockSpec(memory_space=pltpu.VMEM), pl.BlockSpec(memory_space=pl.ANY)
        land_in = jax.ShapeDtypeStruct((CORES, nz, 2, width, ff), jnp.bfloat16)
        land_out = jax.ShapeDtypeStruct((CORES, nz, 2, ff, width), jnp.bfloat16)
        dma = pltpu.SemaphoreType.DMA
        return pl.pallas_call(
            functools.partial(kernel, nz, yspan),
            out_shape=(jax.ShapeDtypeStruct(x_in.shape, x_in.dtype), land_in, land_in, land_out),
            in_specs=[vmem, vmem, vmem, vmem, anywhere, anywhere, anywhere],
            out_specs=(vmem, anywhere, anywhere, anywhere),
            scratch_shapes=[
                pltpu.VMEM((tokens, width), jnp.bfloat16),
                pltpu.VMEM((tokens, width), jnp.float32),
                pltpu.VMEM((experts, tokens, LANES), jnp.float32),
                pltpu.VMEM((tokens, ff), jnp.bfloat16),
                pltpu.VMEM((2, width, ff), jnp.bfloat16),
                pltpu.VMEM((2, width, ff), jnp.bfloat16),
                pltpu.VMEM((2, ff, width), jnp.bfloat16),
                dma((2, 3, batches)),
                dma((2, 3, batches)),
                dma((3, nz, 2)),
                dma((3, CORES, nz, 2)),
                dma((3,)),
            ],
            compiler_params=pltpu.CompilerParams(collective_id=0, has_side_effects=True, vmem_limit_bytes=60 * 1024 * 1024),
            name="moe",
        )(x_in, norm_gain.reshape(1, width), w_router, expert_ids, w_gate, w_up, w_down)[0]

    tok_spec = P(("dp", "ep"), None)
    expert_spec = P("ep", None, None)
    return jax.shard_map(local_block, mesh=mesh, in_specs=(tok_spec, P(None), P(None, None), tok_spec, expert_spec, expert_spec, expert_spec), out_specs=tok_spec, check_vma=False)
```

```python
import functools
import math

import jax
import jax.numpy as jnp
from jax import lax
from jax.experimental import pallas as pl
from jax.experimental.pallas import tpu as pltpu
from jax.sharding import PartitionSpec as P

EPS = 1e-6
MESH = pl.DeviceIdType.MESH
CORES = 2
LAG_FROM_Z, LAG_FROM_XY = 2, 4
DEFER = 2


def kernel(nz, yspan, x_ref, gain_ref, router_ref, ids_ref, gate_in, up_in, down_in, out_ref, gate_land, up_land, down_land,
           normed, total, weight, hidden, gate_buf, up_buf, down_buf, send_z, send_xy, send_sib, recv, load_sem):
    dp, ep = lax.axis_index("dp"), lax.axis_index("ep")
    z, c = ep // CORES, ep % CORES
    a, b = (dp // yspan) % 2, dp % 2
    relay = (a + b + c) % 2
    right = (dp, ((z + 1) % nz) * CORES + c)
    left = (dp, ((z + nz - 1) % nz) * CORES + c)
    x_peer = (dp + yspan * (1 - 2 * a), ep)
    y_peer = (dp + 1 - 2 * b, ep)
    sibling = (dp, z * CORES + 1 - c)
    tokens, width = x_ref.shape
    experts = router_ref.shape[0]
    batches = nz - 1
    items = 4 * nz
    arrays = ((gate_in, gate_land, gate_buf), (up_in, up_land, up_buf), (down_in, down_land, down_buf))

    def send(src, dst, send_sem, recv_sem, device):
        return pltpu.make_async_remote_copy(src_ref=src, dst_ref=dst, send_sem=send_sem, recv_sem=recv_sem, device_id=device, device_id_type=MESH)

    barrier = pltpu.get_barrier_semaphore()
    for peer in (right, left, x_peer, y_peer, sibling):
        pl.semaphore_signal(barrier, inc=1, device_id=peer, device_id_type=MESH)
    pl.semaphore_wait(barrier, 5)

    for j in range(2):
        for k, (own, land, _) in enumerate(arrays):
            @pl.when(relay == 0)
            def _():
                send(own.at[j], land.at[c, z, j], send_z.at[0, k, j], recv.at[k, c, z, j], right).start()
                send(own.at[1 - j], land.at[c, z, 1 - j], send_z.at[1, k, j], recv.at[k, c, z, 1 - j], left).start()
            send(own.at[j], land.at[c, z, j], send_sib.at[k, 0, j], recv.at[k, c, z, j], sibling).start()

    tile = min(128, tokens)

    @pl.loop(0, tokens // tile)
    def _(step):
        rows = pl.ds(pl.multiple_of(step * tile, tile), tile)
        resid = x_ref[rows, :].astype(jnp.float32)
        mean_sq = jnp.mean(resid * resid, axis=-1, keepdims=True)
        row = (resid * lax.rsqrt(mean_sq + EPS) * gain_ref[...].astype(jnp.float32).reshape(1, width)).astype(jnp.bfloat16)
        normed[rows, :] = row
        total[rows, :] = resid
        logits = lax.dot_general(router_ref[...], row, (((1,), (1,)), ((), ())), preferred_element_type=jnp.float32)
        ids = ids_ref[:, rows]
        index = lax.broadcasted_iota(jnp.int32, (experts, tile), 0)
        chosen = index == ids[0:1, :]
        for j in range(1, ids.shape[0]):
            chosen = chosen | (index == ids[j:j + 1, :])
        shifted = jnp.exp(logits - jnp.max(logits, axis=0, keepdims=True))
        prob = shifted / jnp.sum(shifted, axis=0, keepdims=True)
        picked = jnp.where(chosen, prob, 0.0)
        gates = picked / jnp.sum(picked, axis=0, keepdims=True)
        weight[rows, :] = gates.T

    def place(n, side):
        dist, first = 1 + n // 2, n % 2
        return (z + nz + (2 * side - 1) * dist) % nz, first + side - 2 * first * side

    def exchange(n, k):
        _, land, _ = arrays[k]
        first = n % 2
        for side in range(2):
            zs, j = place(n, side)
            chunk, sem = land.at[c, zs, j], recv.at[k, c, zs, j]
            send(chunk, chunk, send_sib.at[k, n + 1, side], sem, sibling).wait_recv()

            @pl.when((relay == 0) & (n < batches - 2))
            def _():
                send(chunk, chunk, send_z.at[side, k, n + 2], sem, (right, left)[side]).start()

            @pl.when((relay == 0) & (first == side))
            def _():
                send(chunk, chunk, send_xy.at[0, k, n], sem, x_peer).start()

            @pl.when((relay == 0) & (first != side))
            def _():
                send(chunk, chunk, send_xy.at[1, k, n], sem, y_peer).start()
            send(chunk, chunk, send_sib.at[k, n + 1, side], sem, sibling).start()

    @pl.when(relay == 0)
    def _():
        exchange(0, 0)

    def locate(i):
        m, q = i // 4, i % 4
        side, other = q % 2, (q // 2 + relay) % 2
        dist, first = (m + 1) // 2, (m + 1) % 2
        return other, (m == 0) & (other == 0), (c + other) % 2, (z + nz + (2 * side - 1) * dist) % nz, first + side - 2 * first * side

    def fetch(i, which):
        other, native, cls, zs, j = locate(i)

        @pl.when(other == 1)
        def _():
            for k in which:
                chunk = arrays[k][1].at[cls, zs, j]
                send(chunk, chunk, send_sib.at[k, 0, 0], recv.at[k, cls, zs, j], sibling).wait_recv()

        @pl.when(native)
        def _():
            for k in which:
                own, _, buf = arrays[k]
                pltpu.make_async_copy(own.at[j], buf.at[i % 2], load_sem.at[k]).start()

        @pl.when(jnp.logical_not(native))
        def _():
            for k in which:
                _, land, buf = arrays[k]
                pltpu.make_async_copy(land.at[cls, zs, j], buf.at[i % 2], load_sem.at[k]).start()

    def fetched(i, which):
        for k in which:
            own, _, buf = arrays[k]
            pltpu.make_async_copy(own.at[0], buf.at[i % 2], load_sem.at[k]).wait()

    span = min(512, tokens)

    @pl.loop(0, items + DEFER)
    def _(i):
        at = i - LAG_FROM_Z - (LAG_FROM_XY - LAG_FROM_Z) * relay
        live = (at >= 1 - relay) & (at < 4 * batches)
        for k, phase in enumerate((0, 2, 3)):
            @pl.when(live & ((at + 8) % 4 == phase))
            def _():
                exchange((at + 8) // 4 - 2, k)

        late = i - DEFER

        @pl.when(late >= 0)
        def _():
            fetch(late, (2,))

        @pl.when(i < items)
        def _():
            fetch(i, (0, 1))
            fetched(i, (0, 1))

            @pl.loop(0, tokens // span)
            def _(step):
                rows = pl.ds(pl.multiple_of(step * span, span), span)
                row = normed[rows, :]
                gate_val = jnp.dot(row, gate_buf[i % 2], preferred_element_type=jnp.float32)
                up_val = jnp.dot(row, up_buf[i % 2], preferred_element_type=jnp.float32)
                hidden[i % 4, rows, :] = (jax.nn.silu(gate_val) * up_val).astype(jnp.bfloat16)

        @pl.when(late >= 0)
        def _():
            fetched(late, (2,))
            _, _, cls, zs, j = locate(late)
            expert = (zs * CORES + cls) * 2 + j

            @pl.loop(0, tokens // span)
            def _(step):
                rows = pl.ds(pl.multiple_of(step * span, span), span)
                y = jnp.dot(hidden[late % 4, rows, :], down_buf[late % 2], preferred_element_type=jnp.float32).astype(jnp.bfloat16).astype(jnp.float32)
                lane = lax.broadcasted_iota(jnp.int32, (span, experts), 1)
                scale = jnp.sum(jnp.where(lane == expert, weight[rows, :], 0.0), axis=1, keepdims=True)
                total[rows, :] += jnp.where(scale != 0.0, scale * y, 0.0)

    @pl.loop(0, tokens // tile)
    def _(step):
        rows = pl.ds(pl.multiple_of(step * tile, tile), tile)
        out_ref[rows, :] = total[rows, :].astype(jnp.bfloat16)

    for k, (own, land, _) in enumerate(arrays):
        @pl.when(relay == 0)
        def _():
            @pl.loop(0, batches)
            def _(n):
                for side in range(2):
                    send(own.at[0], land.at[0, 0, 0], send_z.at[side, k, n], recv.at[k, 0, 0, 0], right).wait_send()
                    send(own.at[0], land.at[0, 0, 0], send_xy.at[side, k, n], recv.at[k, 0, 0, 0], right).wait_send()

        @pl.loop(0, batches + 1)
        def _(n):
            for side in range(2):
                send(own.at[0], land.at[0, 0, 0], send_sib.at[k, n, side], recv.at[k, 0, 0, 0], sibling).wait_send()


def solution(mesh):
    yspan = math.isqrt(mesh.shape["dp"])
    nz = mesh.shape["ep"] // CORES

    def local_block(x_in, norm_gain, w_router, expert_ids, w_gate, w_up, w_down):
        tokens, width = x_in.shape
        experts, ff = w_router.shape[1], w_gate.shape[2]
        batches = nz - 1
        vmem, anywhere = pl.BlockSpec(memory_space=pltpu.VMEM), pl.BlockSpec(memory_space=pl.ANY)
        land_in = jax.ShapeDtypeStruct((CORES, nz, 2, width, ff), jnp.bfloat16)
        land_out = jax.ShapeDtypeStruct((CORES, nz, 2, ff, width), jnp.bfloat16)
        dma = pltpu.SemaphoreType.DMA
        return pl.pallas_call(
            functools.partial(kernel, nz, yspan),
            out_shape=(pltpu.VMEM(x_in.shape, x_in.dtype), land_in, land_in, land_out),
            in_specs=[vmem, vmem, vmem, vmem, anywhere, anywhere, anywhere],
            out_specs=(vmem, anywhere, anywhere, anywhere),
            scratch_shapes=[
                pltpu.VMEM((tokens, width), jnp.bfloat16),
                pltpu.VMEM((tokens, width), jnp.float32),
                pltpu.VMEM((tokens, experts), jnp.float32),
                pltpu.VMEM((4, tokens, ff), jnp.bfloat16),
                pltpu.VMEM((2, width, ff), jnp.bfloat16),
                pltpu.VMEM((2, width, ff), jnp.bfloat16),
                pltpu.VMEM((2, ff, width), jnp.bfloat16),
                dma((2, 3, batches)),
                dma((2, 3, batches)),
                dma((3, nz, 2)),
                dma((3, CORES, nz, 2)),
                dma((3,)),
            ],
            compiler_params=pltpu.CompilerParams(collective_id=0, has_side_effects=True, vmem_limit_bytes=60 * 1024 * 1024),
            name="moe",
        )(x_in, norm_gain, w_router.T, expert_ids.T, w_gate, w_up, w_down)[0]

    tok_spec = P(("dp", "ep"), None)
    expert_spec = P("ep", None, None)
    return jax.shard_map(local_block, mesh=mesh, in_specs=(tok_spec, P(None), P(None, None), tok_spec, expert_spec, expert_spec, expert_spec), out_specs=tok_spec, check_vma=False)
```

```python
import functools
import math

import jax
import jax.numpy as jnp
from jax import lax
from jax.experimental import pallas as pl
from jax.experimental.pallas import tpu as pltpu
from jax.sharding import PartitionSpec as P

EPS = 1e-6
MESH = pl.DeviceIdType.MESH
CORES = 2
DEFER = 4
XY_LAG = 2


def step_times(nz):
    whole = nz // 2 - 1
    slots = 6 * whole + 3
    times = [0, 0, 1, 1]
    for dist in range(1, whole + 1):
        times += [6 * dist - 3] * 2 + [6 * dist - 2] * 2 + [6 * dist - 1] * 2 + [6 * dist] * 2
    return times + [slots - 2] * 2 + [slots] * 4 + [slots + 1] * 2


def kernel(nz, yspan, x_ref, gain_ref, router_ref, ids_ref, gate_in, up_in, down_in, out_ref, gate_land, up_land, down_land,
           normed, total, weight, hidden, gate_buf, up_buf, down_buf, send_z, send_xy, send_sib, recv, recv_sib, load_sem):
    dp, ep = lax.axis_index("dp"), lax.axis_index("ep")
    z, c = ep // CORES, ep % CORES
    a, b = (dp // yspan) % 2, dp % 2
    p = (a + b) % 2
    right = (dp, ((z + 1) % nz) * CORES + c)
    left = (dp, ((z + nz - 1) % nz) * CORES + c)
    x_peer = (dp + yspan * (1 - 2 * a), ep)
    y_peer = (dp + 1 - 2 * b, ep)
    sibling = (dp, z * CORES + 1 - c)
    tokens, width = x_ref.shape
    experts = router_ref.shape[0]
    whole = nz // 2 - 1
    slots = 6 * whole + 3
    items = 4 * nz
    arrays = ((gate_in, gate_land, gate_buf), (up_in, up_land, up_buf), (down_in, down_land, down_buf))

    def send(src, dst, send_sem, recv_sem, device):
        return pltpu.make_async_remote_copy(src_ref=src, dst_ref=dst, send_sem=send_sem, recv_sem=recv_sem, device_id=device, device_id_type=MESH)

    def rows_of(k, piece):
        half = arrays[k][0].shape[1] // 2
        return pl.ds(pl.multiple_of(piece * half, half), half)

    barrier = pltpu.get_barrier_semaphore()
    for peer in (right, left, x_peer, y_peer, sibling):
        pl.semaphore_signal(barrier, inc=1, device_id=peer, device_id_type=MESH)
    pl.semaphore_wait(barrier, 5)

    for k, (own, land, _) in enumerate(arrays):
        for piece in range(2):
            part = rows_of(k, piece)
            for side, peer in enumerate((right, left)):
                send(own.at[p, part], land.at[c, z, p, part], send_z.at[side, 2 * k + piece], recv.at[k, piece, z, p], peer).start()
    for j in range(2):
        for k, (own, land, _) in enumerate(arrays):
            send(own.at[j], land.at[c, z, j], send_sib.at[k, z, j], recv_sib.at[k, z, j], sibling).start()

    tile = min(128, tokens)

    @pl.loop(0, tokens // tile)
    def _(step):
        rows = pl.ds(pl.multiple_of(step * tile, tile), tile)
        resid = x_ref[rows, :].astype(jnp.float32)
        mean_sq = jnp.mean(resid * resid, axis=-1, keepdims=True)
        row = (resid * lax.rsqrt(mean_sq + EPS) * gain_ref[...].astype(jnp.float32).reshape(1, width)).astype(jnp.bfloat16)
        normed[rows, :] = row
        total[rows, :] = resid
        logits = lax.dot_general(router_ref[...], row, (((1,), (1,)), ((), ())), preferred_element_type=jnp.float32)
        ids = ids_ref[:, rows]
        index = lax.broadcasted_iota(jnp.int32, (experts, tile), 0)
        chosen = index == ids[0:1, :]
        for j in range(1, ids.shape[0]):
            chosen = chosen | (index == ids[j:j + 1, :])
        shifted = jnp.exp(logits - jnp.max(logits, axis=0, keepdims=True))
        prob = shifted / jnp.sum(shifted, axis=0, keepdims=True)
        picked = jnp.where(chosen, prob, 0.0)
        gates = picked / jnp.sum(picked, axis=0, keepdims=True)
        weight[rows, :] = gates.T

    def source(side, dist):
        return (z + nz + (2 * side - 1) * dist) % nz

    def take(u, j, from_z):
        is_whole = u < 6 * whole
        at = jnp.where(is_whole, (u % 6) // 2, u - 6 * whole)
        dist = jnp.where(is_whole, 1 + u // 6, whole + 1)
        for k, (own, land, _) in enumerate(arrays):
            @pl.when((u >= 0) & (u < slots) & (at == k))
            def _():
                for side in range(2):
                    zs = source(side, dist)
                    piece = jnp.where(is_whole, u % 2, side)
                    chunk, sem = land.at[c, zs, j, rows_of(k, piece)], recv.at[k, piece, zs, j]
                    send(chunk, chunk, send_z.at[side, u], sem, sibling).wait_recv()
                    if from_z:
                        early = u < 6 * (whole - 1)

                        @pl.when(early | (is_whole & (u % 2 == side)))
                        def _():
                            later = jnp.where(early, u + 6, 6 * whole + (u - 6 * (whole - 1)) // 2)
                            send(chunk, chunk, send_z.at[side, later], sem, (right, left)[side]).start()
                        send(chunk, chunk, send_xy.at[side, u], sem, (x_peer, y_peer)[side]).start()
                for side in range(2):
                    zs = source(side, dist)

                    @pl.when((is_whole & (u % 2 == 1)) | (jnp.logical_not(is_whole) & (side == 0)))
                    def _():
                        send(land.at[c, zs, j], land.at[c, zs, j], send_sib.at[k, zs, j], recv_sib.at[k, zs, j], sibling).start()

    def locate(i):
        m, q = (i + 4) // 8, (i + 4) % 8
        first, last = i < 4, i >= items - 4
        side = q % 2
        other = jnp.where(first, (q - 4) // 2, jnp.where(last, q % 2, (q // 2) % 2))
        dist = jnp.where(first, 0, jnp.where(last, whole + 1, m))
        j = jnp.where(first, side, (p + jnp.where(last, q // 2, q // 4)) % 2)
        return other, first & (other == 0), (c + other) % 2, source(jnp.where(last, 0, side), dist), j

    def fetch(i, which):
        other, native, cls, zs, j = locate(i)

        @pl.when(other == 1)
        def _():
            for k in which:
                own, land, _ = arrays[k]
                send(own.at[0], land.at[cls, zs, j], send_sib.at[k, zs, j], recv_sib.at[k, zs, j], sibling).wait_recv()

        @pl.when(native)
        def _():
            for k in which:
                own, _, buf = arrays[k]
                pltpu.make_async_copy(own.at[j], buf.at[i % 2], load_sem.at[k, i % 2]).start()

        @pl.when(jnp.logical_not(native))
        def _():
            for k in which:
                _, land, buf = arrays[k]
                pltpu.make_async_copy(land.at[cls, zs, j], buf.at[i % 2], load_sem.at[k, i % 2]).start()

    def fetched(i, which):
        for k in which:
            own, _, buf = arrays[k]
            pltpu.make_async_copy(own.at[0], buf.at[i % 2], load_sem.at[k, i % 2]).wait()

    span = min(512, tokens)
    times = step_times(nz)

    def steps_before(v):
        return sum(jnp.where(v > t, times.count(t), 0) for t in sorted(set(times)))

    @pl.loop(0, slots + XY_LAG)
    def _(v):
        take(v, p, True)
        take(v - XY_LAG, 1 - p, False)
        begin, end = steps_before(v), steps_before(v + 1)

        @pl.loop(begin, end)
        def _(i):
            late = i - DEFER

            @pl.when((i == begin) & (i < items))
            def _():
                fetch(i, (0, 1))

            @pl.when(late >= 0)
            def _():
                fetch(late, (2,))

            @pl.when(i < items)
            def _():
                fetched(i, (0, 1))

                @pl.loop(0, tokens // span)
                def _(step):
                    rows = pl.ds(pl.multiple_of(step * span, span), span)
                    row = normed[rows, :]
                    gate_val = jnp.dot(row, gate_buf[i % 2], preferred_element_type=jnp.float32)
                    up_val = jnp.dot(row, up_buf[i % 2], preferred_element_type=jnp.float32)
                    hidden[i % (2 * DEFER), rows, :] = (jax.nn.silu(gate_val) * up_val).astype(jnp.bfloat16)

            @pl.when((i + 1 < end) & (i + 1 < items))
            def _():
                fetch(i + 1, (0, 1))

            @pl.when(late >= 0)
            def _():
                fetched(late, (2,))
                _, _, cls, zs, j = locate(late)
                expert = (zs * CORES + cls) * 2 + j

                @pl.loop(0, tokens // span)
                def _(step):
                    rows = pl.ds(pl.multiple_of(step * span, span), span)
                    y = jnp.dot(hidden[late % (2 * DEFER), rows, :], down_buf[late % 2], preferred_element_type=jnp.float32).astype(jnp.bfloat16).astype(jnp.float32)
                    lane = lax.broadcasted_iota(jnp.int32, (span, experts), 1)
                    scale = jnp.sum(jnp.where(lane == expert, weight[rows, :], 0.0), axis=1, keepdims=True)
                    total[rows, :] += jnp.where(scale != 0.0, scale * y, 0.0)

    @pl.loop(0, tokens // tile)
    def _(step):
        rows = pl.ds(pl.multiple_of(step * tile, tile), tile)
        out_ref[rows, :] = total[rows, :].astype(jnp.bfloat16)

    half = gate_in.at[0, rows_of(0, 0)]

    @pl.loop(0, slots)
    def _(u):
        for side in range(2):
            send(half, half, send_z.at[side, u], recv.at[0, 0, 0, 0], right).wait_send()
            send(half, half, send_xy.at[side, u], recv.at[0, 0, 0, 0], right).wait_send()

    @pl.loop(0, nz)
    def _(zs):
        for k, (own, land, _) in enumerate(arrays):
            for j in range(2):
                send(own.at[0], land.at[0, 0, 0], send_sib.at[k, zs, j], recv_sib.at[k, 0, 0], sibling).wait_send()


def solution(mesh):
    yspan = math.isqrt(mesh.shape["dp"])
    nz = mesh.shape["ep"] // CORES

    def local_block(x_in, norm_gain, w_router, expert_ids, w_gate, w_up, w_down):
        tokens, width = x_in.shape
        experts, ff = w_router.shape[1], w_gate.shape[2]
        slots = 6 * (nz // 2 - 1) + 3
        vmem, anywhere = pl.BlockSpec(memory_space=pltpu.VMEM), pl.BlockSpec(memory_space=pl.ANY)
        land_in = jax.ShapeDtypeStruct((CORES, nz, 2, width, ff), jnp.bfloat16)
        land_out = jax.ShapeDtypeStruct((CORES, nz, 2, ff, width), jnp.bfloat16)
        dma = pltpu.SemaphoreType.DMA
        return pl.pallas_call(
            functools.partial(kernel, nz, yspan),
            out_shape=(pltpu.VMEM(x_in.shape, x_in.dtype), land_in, land_in, land_out),
            in_specs=[vmem, vmem, vmem, vmem, anywhere, anywhere, anywhere],
            out_specs=(vmem, anywhere, anywhere, anywhere),
            scratch_shapes=[
                pltpu.VMEM((tokens, width), jnp.bfloat16),
                pltpu.VMEM((tokens, width), jnp.float32),
                pltpu.VMEM((tokens, experts), jnp.float32),
                pltpu.VMEM((2 * DEFER, tokens, ff), jnp.bfloat16),
                pltpu.VMEM((2, width, ff), jnp.bfloat16),
                pltpu.VMEM((2, width, ff), jnp.bfloat16),
                pltpu.VMEM((2, ff, width), jnp.bfloat16),
                dma((2, slots)),
                dma((2, slots)),
                dma((3, nz, 2)),
                dma((3, 2, nz, 2)),
                dma((3, nz, 2)),
                dma((3, 2)),
            ],
            compiler_params=pltpu.CompilerParams(collective_id=0, has_side_effects=True, vmem_limit_bytes=60 * 1024 * 1024),
            name="moe",
        )(x_in, norm_gain, w_router.T, expert_ids.T, w_gate, w_up, w_down)[0]

    tok_spec = P(("dp", "ep"), None)
    expert_spec = P("ep", None, None)
    return jax.shard_map(local_block, mesh=mesh, in_specs=(tok_spec, P(None), P(None, None), tok_spec, expert_spec, expert_spec, expert_spec), out_specs=tok_spec, check_vma=False)
```

```python
import functools
import math

import jax
import jax.numpy as jnp
from jax import lax
from jax.experimental import pallas as pl
from jax.experimental.pallas import tpu as pltpu
from jax.sharding import PartitionSpec as P

EPS = 1e-6
MESH = pl.DeviceIdType.MESH
CORES = 2
DEFER = 4
XY_LAG = 2


def step_times(nz):
    whole = nz // 2 - 1
    slots = 6 * whole + 3
    times = [0, 0, 1, 2]
    for dist in range(1, whole + 1):
        spread = (0, 1, 2, 2, 3, 4, 4, 5) if dist < whole else (0, 0, 1, 1, 2, 2, 3, 3)
        times += [6 * dist - 3 + after for after in spread]
    return times + [slots - 2] * 3 + [slots - 1] * 2 + [slots] * 2 + [slots + 1] * 2


def kernel(nz, yspan, x_ref, gain_ref, router_ref, ids_ref, gate_in, up_in, down_in, out_ref, gate_land, up_land, down_land,
           normed, total, weight, hidden, gate_buf, up_buf, down_buf, x_buf, send_z, send_xy, send_sib, send_extra, recv, recv_sib, recv_extra, load_sem, x_sem):
    dp, ep = lax.axis_index("dp"), lax.axis_index("ep")
    z, c = ep // CORES, ep % CORES
    a, b = (dp // yspan) % 2, dp % 2
    p = (a + b) % 2
    right = (dp, ((z + 1) % nz) * CORES + c)
    left = (dp, ((z + nz - 1) % nz) * CORES + c)
    x_peer = (dp + yspan * (1 - 2 * a), ep)
    y_peer = (dp + 1 - 2 * b, ep)
    sibling = (dp, z * CORES + 1 - c)
    tokens, width = x_ref.shape
    experts = router_ref.shape[0]
    whole = nz // 2 - 1
    slots = 6 * whole + 3
    items = 4 * nz
    arrays = ((gate_in, gate_land, gate_buf), (up_in, up_land, up_buf), (down_in, down_land, down_buf))

    def send(src, dst, send_sem, recv_sem, device):
        return pltpu.make_async_remote_copy(src_ref=src, dst_ref=dst, send_sem=send_sem, recv_sem=recv_sem, device_id=device, device_id_type=MESH)

    def rows_of(k, piece):
        half = arrays[k][0].shape[1] // 2
        return pl.ds(pl.multiple_of(piece * half, half), half)

    x_load = pltpu.make_async_copy(x_ref, x_buf, x_sem)
    x_load.start()
    def quarter(piece, part):
        size = down_in.shape[1] // 4
        return pl.ds((2 * piece + part) * size, size)

    barrier = pltpu.get_barrier_semaphore()
    for peer in (right, left, x_peer, y_peer, sibling):
        pl.semaphore_signal(barrier, inc=1, device_id=peer, device_id_type=MESH)
    pl.semaphore_wait(barrier, 5)

    for k, (own, land, _) in enumerate(arrays):
        for piece in range(2):
            part = rows_of(k, piece)
            for side, peer in enumerate((right, left)):
                send(own.at[p, part], land.at[c, z, p, part], send_z.at[side, 2 * k + piece], recv.at[k, piece, z, p], peer).start()
    for j in range(2):
        for k, (own, land, _) in enumerate(arrays):
            send(own.at[j], land.at[c, z, j], send_sib.at[k, z, j], recv_sib.at[k, z, j], sibling).start()

    tile = min(128, tokens)
    x_load.wait()

    @pl.loop(0, tokens // tile)
    def _(step):
        rows = pl.ds(pl.multiple_of(step * tile, tile), tile)
        resid = x_buf[rows, :].astype(jnp.float32)
        mean_sq = jnp.mean(resid * resid, axis=-1, keepdims=True)
        row = (resid * lax.rsqrt(mean_sq + EPS) * gain_ref[...].astype(jnp.float32).reshape(1, width)).astype(jnp.bfloat16)
        normed[rows, :] = row
        total[rows, :] = resid
        logits = lax.dot_general(router_ref[...], row, (((1,), (1,)), ((), ())), preferred_element_type=jnp.float32)
        ids = ids_ref[:, rows]
        index = lax.broadcasted_iota(jnp.int32, (experts, tile), 0)
        chosen = index == ids[0:1, :]
        for j in range(1, ids.shape[0]):
            chosen = chosen | (index == ids[j:j + 1, :])
        shifted = jnp.exp(logits - jnp.max(logits, axis=0, keepdims=True))
        prob = shifted / jnp.sum(shifted, axis=0, keepdims=True)
        picked = jnp.where(chosen, prob, 0.0)
        gates = picked / jnp.sum(picked, axis=0, keepdims=True)
        weight[rows, :] = gates.T

    def source(side, dist):
        return (z + nz + (2 * side - 1) * dist) % nz

    def take(u, j, from_z):
        is_whole = u < 6 * whole
        at = jnp.where(is_whole, (u % 6) // 2, u - 6 * whole)
        dist = jnp.where(is_whole, 1 + u // 6, whole + 1)
        for k, (own, land, _) in enumerate(arrays):
            @pl.when((u >= 0) & (u < slots - 1) & (at == k))
            def _():
                for side in range(2):
                    zs = source(side, dist)
                    piece = jnp.where(is_whole, u % 2, side)
                    chunk, sem = land.at[c, zs, j, rows_of(k, piece)], recv.at[k, piece, zs, j]
                    send(chunk, chunk, send_z.at[side, u], sem, sibling).wait_recv()
                    if from_z:
                        early = u < 6 * (whole - 1)

                        @pl.when(early | (is_whole & (u % 2 == side)))
                        def _():
                            later = jnp.where(early, u + 6, 6 * whole + (u - 6 * (whole - 1)) // 2)
                            send(chunk, chunk, send_z.at[side, later], sem, (right, left)[side]).start()
                        send(chunk, chunk, send_xy.at[side, u], sem, (x_peer, y_peer)[side]).start()
                for side in range(2):
                    zs = source(side, dist)

                    @pl.when((is_whole & (u % 2 == 1)) | (jnp.logical_not(is_whole) & (side == 0)))
                    def _():
                        send(land.at[c, zs, j], land.at[c, zs, j], send_sib.at[k, zs, j], recv_sib.at[k, zs, j], sibling).start()

    def take_last(j, from_z):
        _, land, _ = arrays[2]
        zs = source(0, whole + 1)

        def share(part):
            send(part, part, send_sib.at[2, zs, j], recv_sib.at[2, zs, j], sibling).start()

        for side in range(2):
            sem, first = recv.at[2, side, zs, j], land.at[c, zs, j, quarter(side, 0)]
            if from_z:
                chunk = land.at[c, zs, j, rows_of(2, side)]
                send(chunk, chunk, send_z.at[side, 0], sem, sibling).wait_recv()
                send(first, first, send_xy.at[side, slots - 1], sem, (x_peer, y_peer)[side]).start()
                extra = land.at[c, source(side, whole), 1 - j, quarter(side, 1)]
                send(extra, extra, send_extra.at[side], recv_extra.at[side], (right, left)[side]).start()
                share(chunk)
            else:
                send(first, first, send_z.at[side, 0], sem, sibling).wait_recv()
                share(first)
        if not from_z:
            for side in range(2):
                second = land.at[c, zs, j, quarter(side, 1)]
                send(second, second, send_z.at[side, 0], recv_extra.at[side], sibling).wait_recv()
                share(second)

    def locate(i):
        m, q = (i + 4) // 8, (i + 4) % 8
        first, last = i < 4, i >= items - 4
        side = q % 2
        other = jnp.where(first, (q - 4) // 2, jnp.where(last, q % 2, (q // 2) % 2))
        dist = jnp.where(first, 0, jnp.where(last, whole + 1, m))
        j = jnp.where(first, side, (p + jnp.where(last, q // 2, q // 4)) % 2)
        return other, first & (other == 0), (c + other) % 2, source(jnp.where(last, 0, side), dist), j

    def fetch(i, which):
        other, native, cls, zs, j = locate(i)

        @pl.when(other == 1)
        def _():
            for k in which:
                own, land, _ = arrays[k]
                send(own.at[0], land.at[cls, zs, j], send_sib.at[k, zs, j], recv_sib.at[k, zs, j], sibling).wait_recv()

        @pl.when(native)
        def _():
            for k in which:
                own, _, buf = arrays[k]
                pltpu.make_async_copy(own.at[j], buf.at[i % 2], load_sem.at[k, i % 2]).start()

        @pl.when(jnp.logical_not(native))
        def _():
            for k in which:
                _, land, buf = arrays[k]
                pltpu.make_async_copy(land.at[cls, zs, j], buf.at[i % 2], load_sem.at[k, i % 2]).start()

    def fetched(i, which):
        for k in which:
            own, _, buf = arrays[k]
            pltpu.make_async_copy(own.at[0], buf.at[i % 2], load_sem.at[k, i % 2]).wait()

    span = min(1024, tokens)
    times = step_times(nz)

    def steps_before(v):
        return sum(jnp.where(v > t, times.count(t), 0) for t in sorted(set(times)))

    @pl.loop(0, slots + XY_LAG)
    def _(v):
        take(v, p, True)

        @pl.when(v == slots - 1)
        def _():
            take_last(p, True)
        take(v - XY_LAG, 1 - p, False)

        @pl.when(v - XY_LAG == slots - 1)
        def _():
            take_last(1 - p, False)
        begin, end = steps_before(v), steps_before(v + 1)

        @pl.loop(begin, end)
        def _(step):
            tail = step - (items - 4)
            i = jnp.where(tail <= 0, step, jnp.where(tail == 3, items - 3, step - 3))
            early = (tail <= 0) | (tail == 3) | (tail == 5) | (tail == 6)
            late = jnp.where(tail <= 4, step - DEFER, step - DEFER - 1)
            ripe = (late >= 0) & (tail != 5)

            @pl.when(early & ((tail > 0) | ((step == begin) & (i % 4 == 0))))
            def _():
                fetch(i, (0, 1))

            @pl.when(ripe & (tail != 1) & (tail != 2) & (tail != 4))
            def _():
                fetch(late, (2,))

            @pl.when(early)
            def _():
                fetched(i, (0, 1))

                @pl.loop(0, tokens // span)
                def _(part):
                    rows = pl.ds(pl.multiple_of(part * span, span), span)
                    row = normed[rows, :]
                    gate_val = jnp.dot(row, gate_buf[i % 2], preferred_element_type=jnp.float32)
                    up_val = jnp.dot(row, up_buf[i % 2], preferred_element_type=jnp.float32)
                    hidden[i % (2 * DEFER), rows, :] = (jax.nn.silu(gate_val) * up_val).astype(jnp.bfloat16)

            @pl.when((tail < 0) & ((step + 1 < end) | ((i + 1) % 4 != 0)))
            def _():
                fetch(i + 1, (0, 1))

            @pl.when((tail == 0) | (tail == 1) | (tail == 3))
            def _():
                fetch(late + 1, (2,))

            @pl.when(ripe)
            def _():
                fetched(late, (2,))
                _, _, cls, zs, j = locate(late)
                expert = (zs * CORES + cls) * 2 + j

                @pl.loop(0, tokens // span)
                def _(part):
                    rows = pl.ds(pl.multiple_of(part * span, span), span)
                    y = jnp.dot(hidden[late % (2 * DEFER), rows, :], down_buf[late % 2], preferred_element_type=jnp.float32).astype(jnp.bfloat16).astype(jnp.float32)
                    lane = lax.broadcasted_iota(jnp.int32, (span, experts), 1)
                    scale = jnp.sum(jnp.where(lane == expert, weight[rows, :], 0.0), axis=1, keepdims=True)
                    total[rows, :] += jnp.where(scale != 0.0, scale * y, 0.0)

    @pl.loop(0, tokens // tile)
    def _(step):
        rows = pl.ds(pl.multiple_of(step * tile, tile), tile)
        out_ref[rows, :] = total[rows, :].astype(jnp.bfloat16)

    half = gate_in.at[0, rows_of(0, 0)]

    @pl.loop(0, slots)
    def _(u):
        for side in range(2):
            send(half, half, send_z.at[side, u], recv.at[0, 0, 0, 0], right).wait_send()

            @pl.when(u < slots - 1)
            def _():
                send(half, half, send_xy.at[side, u], recv.at[0, 0, 0, 0], right).wait_send()

    piece = down_in.at[0, quarter(0, 0)]
    for side in range(2):
        send(piece, piece, send_xy.at[side, slots - 1], recv.at[0, 0, 0, 0], right).wait_send()
        send(piece, piece, send_extra.at[side], recv.at[0, 0, 0, 0], right).wait_send()

    @pl.loop(0, nz)
    def _(zs):
        for k, (own, land, _) in enumerate(arrays):
            for j in range(2):
                send(own.at[0], land.at[0, 0, 0], send_sib.at[k, zs, j], recv_sib.at[k, 0, 0], sibling).wait_send()


def solution(mesh):
    yspan = math.isqrt(mesh.shape["dp"])
    nz = mesh.shape["ep"] // CORES

    def local_block(x_in, norm_gain, w_router, expert_ids, w_gate, w_up, w_down):
        tokens, width = x_in.shape
        experts, ff = w_router.shape[1], w_gate.shape[2]
        slots = 6 * (nz // 2 - 1) + 3
        vmem, anywhere = pl.BlockSpec(memory_space=pltpu.VMEM), pl.BlockSpec(memory_space=pl.ANY)
        land_in = jax.ShapeDtypeStruct((CORES, nz, 2, width, ff), jnp.bfloat16)
        land_out = jax.ShapeDtypeStruct((CORES, nz, 2, ff, width), jnp.bfloat16)
        dma = pltpu.SemaphoreType.DMA
        return pl.pallas_call(
            functools.partial(kernel, nz, yspan),
            out_shape=(pltpu.VMEM(x_in.shape, x_in.dtype), land_in, land_in, land_out),
            in_specs=[anywhere, vmem, vmem, vmem, anywhere, anywhere, anywhere],
            out_specs=(vmem, anywhere, anywhere, anywhere),
            scratch_shapes=[
                pltpu.VMEM((tokens, width), jnp.bfloat16),
                pltpu.VMEM((tokens, width), jnp.float32),
                pltpu.VMEM((tokens, experts), jnp.float32),
                pltpu.VMEM((2 * DEFER, tokens, ff), jnp.bfloat16),
                pltpu.VMEM((2, width, ff), jnp.bfloat16),
                pltpu.VMEM((2, width, ff), jnp.bfloat16),
                pltpu.VMEM((2, ff, width), jnp.bfloat16),
                pltpu.VMEM((tokens, width), jnp.bfloat16),
                dma((2, slots)),
                dma((2, slots)),
                dma((3, nz, 2)),
                dma((2,)),
                dma((3, 2, nz, 2)),
                dma((3, nz, 2)),
                dma((2,)),
                dma((3, 2)),
                dma(()),
            ],
            compiler_params=pltpu.CompilerParams(collective_id=0, has_side_effects=True, vmem_limit_bytes=60 * 1024 * 1024),
            name="moe",
        )(x_in, norm_gain, w_router.T, expert_ids.T, w_gate, w_up, w_down)[0]

    tok_spec = P(("dp", "ep"), None)
    expert_spec = P("ep", None, None)
    return jax.shard_map(local_block, mesh=mesh, in_specs=(tok_spec, P(None), P(None, None), tok_spec, expert_spec, expert_spec, expert_spec), out_specs=tok_spec, check_vma=False)
```
